512 devices in a mesh: tile: 128 (over z_hi, x, y, core), lev: 4 (over z_lo).
Axes of the slice: x: 4, y: 8, z: 8 (z_hi: 2, z_lo: 4; z = z_hi * 4 + z_lo), core: 2. Of those that a mesh axis runs over, the one named last changes fastest.
Arguments:
- members_pert: bfloat16 [64, 16, 524288], P('lev', None, 'tile'), may hold values from -4 to 4
- coarse_pert: bfloat16 [64, 8, 32768], P('lev', None, 'tile'), may hold values from -6 to 6
- member_ctrl: bfloat16 [64, 16, 32768], P('lev', None, 'tile'), may hold values from -6 to 6
- coarse_ctrl: bfloat16 [64, 8, 32768], P('lev', None, 'tile'), may hold values from -6 to 6
- vert_loc: float32 [64, 64], replicated, may hold values from -1.5 to 1.5, as said below
- stencil: int32 [4, 524288], P(None, 'tile'), may hold values from 0 to 383, as said below
- interp_w: bfloat16 [4, 524288], P(None, 'tile'), may hold values from 0 to 1, as said below
Outputs:
- member_out: float32 [64, 16, 32768], P('lev', None, 'tile')
- coarse_out: float32 [64, 8, 32768], P('lev', None, 'tile')
The draws below stay inside these ranges and needn't reach their ends.
Inputs may be any that keep to these rules, and one draw needn't show every extreme that they name: vert_loc[i, j] is zero where |i - j| > 4, and nonzero where |i - j| = 4. stencil indexes a window of 384 coarse cells of the fine cell's tile index: the last 64 coarse cells of the tile index before it (the first one's predecessor is the last), its own 256 cells, then the first 64 cells of the tile index after it; the four corners of a fine cell are distinct. `interp_w`: the four weights of a fine cell are nonnegative and sum to one up to rounding.
All inputs are finite; a program needn't handle non-finite values.
Results may differ from the reference program's by a relative error of at most 0.013.
Values may be sent and summed in bfloat16 or wider, within the bound.
No kernel may reach another device: no remote copies, remote signals or barrier semaphores. Data moves between devices by JAX's collectives and lax.ppermute only.
A program may use at most 64 MiB of HBM per device.

```python
import jax
import jax.numpy as jnp
from jax import lax

MEMBERS = 16
COARSE_MEMBERS = 8
HB = 4
CW = 64
CR = 4
LEV = 64
NCD = 256
NFD = 4096
NC = 32768
NF = 524288
N_TILE = 128


def draw_vert_loc(key, part):
    first_key, second_key = jax.random.split(key)
    rows = jnp.arange(LEV, dtype=jnp.int32)[:, None]
    columns = jnp.arange(LEV, dtype=jnp.int32)[None, :]
    distance = jnp.abs(rows - columns)
    offdiag = jnp.clip(0.35 * jax.random.normal(first_key, (LEV, LEV), jnp.float32), -1.5, 1.5)
    offdiag = jnp.where(jnp.abs(offdiag) < 0.05, 0.05, offdiag)
    diagonal = 1.0 + jax.random.uniform(second_key, (LEV, LEV), jnp.float32, 0.0, 0.5)
    return jnp.where(distance == 0, diagonal, jnp.where(distance <= HB, offdiag, 0.0)).astype(jnp.float32)


def draw_stencil(key, part):
    row_key, col_key = jax.random.split(key)
    local = jnp.arange(NF, dtype=jnp.int32) % NFD
    fine_row = local // (4 * CW)
    fine_col = local % (4 * CW)
    row_base = jnp.clip((fine_row - 2) // 4 + jax.random.randint(row_key, (NF,), -1, 2), -1, CR - 1)
    col_base = jnp.clip((fine_col - 2) // 4 + jax.random.randint(col_key, (NF,), -1, 2), 0, CW - 2)
    corner = (row_base + 1) * CW + col_base
    return jnp.stack([corner, corner + 1, corner + CW, corner + CW + 1]).astype(jnp.int32)


def draw_interp_w(key, part):
    along_key, across_key = jax.random.split(key)
    along = jax.random.uniform(along_key, (NF,), jnp.float32)
    across = jax.random.uniform(across_key, (NF,), jnp.float32)
    weights = jnp.stack([(1.0 - along) * (1.0 - across), along * (1.0 - across), (1.0 - along) * across, along * across])
    return weights.astype(jnp.bfloat16)


def shard_levels(key, dims, pieces, low, top_value):
    gain = 1.0
    for dim, parts in pieces:
        heights = jax.random.uniform(jax.random.fold_in(jax.random.fold_in(key, 6), dim), (parts,), jnp.float32, low / len(pieces), top_value / len(pieces))
        gain = gain * jnp.repeat(jnp.exp(heights), dims[dim] // parts).reshape((-1,) + (1,) * (len(dims) - 1 - dim))
    return gain


def noise(own_key, shape, spread, reach, shards=(), kind=jnp.bfloat16):
    array = spread * jax.random.normal(own_key, shape, jnp.float32)
    if shards:
        array = array * shard_levels(own_key, shape, shards, -0.22, 0.18)
    return jnp.clip(array, -reach, reach).astype(kind)


def setup_inputs(seed: int = 0) -> dict:
    splits = jax.random.split(jax.random.key(seed), 8)
    members_pert = noise(splits[0], (LEV, MEMBERS, NF), 0.3, 4.0, ((0, 4), (2, 128)))
    coarse_pert = noise(splits[1], (LEV, COARSE_MEMBERS, NC), 0.4, 6.0, ((0, 4), (2, 128)))
    member_ctrl = noise(splits[2], (LEV, MEMBERS, NC), 1.0, 6.0, ((0, 4), (2, 128)))
    coarse_ctrl = noise(splits[3], (LEV, COARSE_MEMBERS, NC), 1.0, 6.0, ((0, 4), (2, 128)))
    vert_loc = draw_vert_loc(jax.random.fold_in(splits[7], 71), 0)
    stencil = draw_stencil(jax.random.fold_in(splits[7], 71), 0)
    interp_w = draw_interp_w(jax.random.fold_in(splits[7], 71), 0)
    return {"members_pert": members_pert, "coarse_pert": coarse_pert, "member_ctrl": member_ctrl, "coarse_ctrl": coarse_ctrl, "vert_loc": vert_loc, "stencil": stencil, "interp_w": interp_w}


def reference(members_pert, coarse_pert, member_ctrl, coarse_ctrl, vert_loc, stencil, interp_w):
    highest = lax.Precision.HIGHEST
    loc_members = jnp.einsum("ij,jkc->ikc", vert_loc, member_ctrl.astype(jnp.float32), precision=highest).astype(jnp.bfloat16)
    loc_coarse = jnp.einsum("ij,jkc->ikc", vert_loc, coarse_ctrl.astype(jnp.float32), precision=highest).astype(jnp.bfloat16)
    combined = jnp.sum(coarse_pert.astype(jnp.float32) * loc_coarse.astype(jnp.float32), axis=1).astype(jnp.bfloat16)
    fields = jnp.concatenate([loc_members, combined[:, None, :]], axis=1)
    levels = fields.shape[0]
    kinds = fields.shape[1]
    blocks = fields.reshape(levels, kinds, N_TILE, NCD)
    window = jnp.concatenate([jnp.roll(blocks, 1, axis=2)[..., NCD - CW:], blocks, jnp.roll(blocks, -1, axis=2)[..., :CW]], axis=3)
    window = jnp.moveaxis(window, 2, 0)
    window_span = window.shape[3]

    def one_tile(tile_index):
        local_window = lax.dynamic_index_in_dim(window, tile_index, 0, keepdims=False)
        first = (tile_index * NFD).astype(jnp.int32)
        corners = lax.dynamic_slice_in_dim(stencil, first, NFD, 1)
        weights = lax.dynamic_slice_in_dim(interp_w, first, NFD, 1).astype(jnp.float32)
        pert = lax.dynamic_slice_in_dim(members_pert, first, NFD, 2).astype(jnp.float32)
        interp = jnp.zeros((levels, kinds, NFD), jnp.float32)
        for corner in range(4):
            interp = interp + weights[corner][None, None, :] * local_window[:, :, corners[corner]].astype(jnp.float32)
        increment = jnp.sum(pert * interp[:, :MEMBERS], axis=1) + interp[:, MEMBERS]
        adjoint = jnp.concatenate([pert * increment[:, None, :], increment[:, None, :]], axis=1)
        adjoint = adjoint.astype(jnp.bfloat16).astype(jnp.float32)
        coarse_adjoint = jnp.zeros((levels, kinds, window_span), jnp.float32)
        for corner in range(4):
            coarse_adjoint = coarse_adjoint.at[:, :, corners[corner]].add(weights[corner][None, None, :] * adjoint)
        return coarse_adjoint

    backs = lax.map(one_tile, jnp.arange(N_TILE, dtype=jnp.int32))
    own_cells = backs[..., CW:CW + NCD]
    left_rim = backs[..., :CW]
    right_rim = backs[..., CW + NCD:]
    own_cells = own_cells.at[..., NCD - CW:].add(jnp.roll(left_rim, -1, axis=0))
    own_cells = own_cells.at[..., :CW].add(jnp.roll(right_rim, 1, axis=0))
    gathered = jnp.moveaxis(own_cells, 0, 2).reshape(levels, kinds, N_TILE * NCD)
    adjoint_ctrl = jnp.concatenate([gathered[:, :MEMBERS], coarse_pert.astype(jnp.float32) * gathered[:, MEMBERS:MEMBERS + 1]], axis=1)
    result = jnp.einsum("ij,ikc->jkc", vert_loc, adjoint_ctrl, precision=highest)
    return result[:, :MEMBERS], result[:, MEMBERS:]
```

```python
import jax
import jax.numpy as jnp
from jax import lax
from jax.experimental import pallas as pl
from jax.experimental.pallas import tpu as pltpu
from jax.sharding import PartitionSpec as P


HB = 4
CW = 64
LV = 16
MB = 16
CM = 8
ND = 256
NF = 4096
WL = LV + 2 * HB
ROWS = LV * MB + LV
HALF = 144
SPAN = ND + 2 * CW
BLOCK = 512
F32 = jnp.float32
BF16 = jnp.bfloat16
SMEM = pl.BlockSpec(memory_space=pltpu.SMEM)
VMEM = pl.BlockSpec(memory_space=pltpu.VMEM)


def low_lanes(shape):
    return lax.broadcasted_iota(jnp.int32, shape, 1) < CW


def turn(value):
    return pltpu.roll(value, CW, 1)


def gather_kernel(mc_hbm, cc_hbm, cp_hbm, stencil_hbm, weight_hbm, top, bottom, mc, cc, cp, stencil, weight, sems):
    moves = [
        (mc_hbm.at[pl.ds(LV - HB, HB)], top.at[:, pl.ds(0, MB)]),
        (cc_hbm.at[pl.ds(LV - HB, HB)], top.at[:, pl.ds(MB, CM)]),
        (mc_hbm.at[pl.ds(0, HB)], bottom.at[:, pl.ds(0, MB)]),
        (cc_hbm.at[pl.ds(0, HB)], bottom.at[:, pl.ds(MB, CM)]),
        (mc_hbm, mc),
        (cc_hbm, cc),
        (cp_hbm, cp),
        (stencil_hbm, stencil),
        (weight_hbm, weight),
    ]
    copies = [pltpu.make_async_copy(source, target, sems.at[k]) for k, (source, target) in enumerate(moves)]
    for copy in copies:
        copy.start()
    for copy in copies:
        copy.wait()


def localize_kernel(odd_ref, band_ref, mc_ref, cc_ref, below_ref, above_ref, cp_ref, own_ref, chip_ref, cross_ref, ms, cs, full):
    for j in range(WL):
        if j < HB:
            ms[j] = below_ref[j, :MB].astype(F32)
            cs[j] = below_ref[j, MB:].astype(F32)
        elif j < HB + LV:
            ms[j] = mc_ref[j - HB].astype(F32)
            cs[j] = cc_ref[j - HB].astype(F32)
        else:
            ms[j] = above_ref[j - HB - LV, :MB].astype(F32)
            cs[j] = above_ref[j - HB - LV, MB:].astype(F32)
    full[ROWS:] = jnp.zeros((2 * HALF - ROWS, ND), F32)
    for i in range(LV):
        member = band_ref[i, i] * ms[i]
        coarse = band_ref[i, i] * cs[i]
        for j in range(i + 1, i + 2 * HB + 1):
            member = member + band_ref[i, j] * ms[j]
            coarse = coarse + band_ref[i, j] * cs[j]
        full[i * MB : (i + 1) * MB] = member
        coarse = coarse.astype(BF16).astype(F32)
        full[LV * MB + i : LV * MB + i + 1] = jnp.sum(cp_ref[i].astype(F32) * coarse, axis=0, keepdims=True)
    own_ref[...] = full[:ROWS].astype(BF16)
    odd = odd_ref[0] == 1
    first = full[:, : 2 * CW]
    last = full[:, ND - 2 * CW :]
    low = low_lanes((HALF, 2 * CW))
    first = jnp.where(low, first[:HALF], turn(first[HALF:]))
    last = jnp.where(low, turn(last[:HALF]), last[HALF:])
    cross_ref[...] = jnp.where(odd, last, first).astype(BF16)
    chip_ref[...] = jnp.where(odd, first, last).astype(BF16)


def weights_kernel(odd_ref, stencil_ref, weight_ref, pert_hbm, out_ref, pert_ref, sem):
    fetch = pltpu.make_async_copy(pert_hbm, pert_ref, sem)
    fetch.start()
    odd = odd_ref[0]
    rows = 16
    for start in range(0, NF, BLOCK):
        span = pl.ds(start, BLOCK)
        row = lax.broadcasted_iota(jnp.int32, (rows, BLOCK), 0)
        cells = [jnp.broadcast_to(stencil_ref[q : q + 1, span], (rows, BLOCK)) - row for q in range(4)]
        weights = [jnp.broadcast_to(weight_ref[q : q + 1, span].astype(F32), (rows, BLOCK)) for q in range(4)]
        for base in range(0, SPAN, rows):
            if base < ND:
                cell = base + CW
            elif base < ND + CW:
                cell = base - ND + (1 - odd) * (ND + CW)
            else:
                cell = base - ND - CW + odd * (ND + CW)
            value = jnp.where(cells[0] == cell, weights[0], 0.0)
            for q in range(1, 4):
                value = jnp.where(cells[q] == cell, weights[q], value)
            out_ref[base : base + rows, span] = value.astype(BF16)
    fetch.wait()


def fine_kernel(own_ref, chip_ref, cross_ref, matrix_ref, pert, own_out, chip_out, cross_out, field):
    chip = chip_ref[...].astype(F32)
    cross = cross_ref[...].astype(F32)
    low = low_lanes((HALF, 2 * CW))
    field[:, :ND] = own_ref[...]
    field[:HALF, ND:] = jnp.where(low, chip, turn(cross)).astype(BF16)
    field[HALF:, ND:] = jnp.where(low, turn(chip), cross)[: ROWS - HALF].astype(BF16)
    total = jnp.zeros((ROWS, SPAN), F32)
    for b in range(NF // BLOCK):
        span = pl.ds(b * BLOCK, BLOCK)
        matrix = matrix_ref[:, span]
        interp = jnp.dot(field[...], matrix, preferred_element_type=F32)
        member = pert[:, span].astype(F32).reshape(LV, MB, BLOCK)
        increment = jnp.sum(member * interp[: LV * MB].reshape(LV, MB, BLOCK), axis=1) + interp[LV * MB :]
        adjoint = (member * increment[:, None, :]).astype(BF16).reshape(LV * MB, BLOCK)
        adjoint = jnp.concatenate([adjoint, increment.astype(BF16)], axis=0)
        total = total + lax.dot_general(adjoint, matrix, (((1,), (1,)), ((), ())), preferred_element_type=F32)
    own_out[...] = total[:, :ND]
    top = total[:HALF, ND:]
    bottom = jnp.concatenate([total[HALF:, ND:], jnp.zeros((2 * HALF - ROWS, 2 * CW), F32)], axis=0)
    chip_out[...] = jnp.where(low, top, turn(bottom)).astype(BF16)
    cross_out[...] = jnp.where(low, turn(top), bottom).astype(BF16)


def spread_kernel(odd_ref, band_ref, own_ref, chip_ref, cross_ref, cp_ref, member_out, coarse_out, down_out, up_out, ms, cs):
    odd = odd_ref[0] == 1
    chip = chip_ref[...].astype(F32)
    cross = cross_ref[...].astype(F32)
    low = low_lanes((HALF, 2 * CW))
    lead = jnp.where(odd, chip, cross)
    trail = jnp.where(odd, cross, chip)
    lead = [jnp.where(low, lead, 0.0), jnp.where(low, turn(lead), 0.0)]
    trail = [jnp.where(low, 0.0, turn(trail)), jnp.where(low, 0.0, trail)]
    lead = jnp.concatenate(lead, axis=0)
    trail = jnp.concatenate(trail, axis=0)
    for i in range(LV):
        rows = slice(i * MB, (i + 1) * MB)
        ms[i, :, : 2 * CW] = own_ref[rows, : 2 * CW] + lead[rows]
        ms[i, :, 2 * CW :] = own_ref[rows, 2 * CW :] + trail[rows]
        row = slice(LV * MB + i, LV * MB + i + 1)
        pert = cp_ref[i].astype(F32)
        cs[i, :, : 2 * CW] = pert[:, : 2 * CW] * (own_ref[row, : 2 * CW] + lead[row])
        cs[i, :, 2 * CW :] = pert[:, 2 * CW :] * (own_ref[row, 2 * CW :] + trail[row])
    for j in range(WL):
        member = None
        for i in range(max(0, j - 2 * HB), min(LV - 1, j) + 1):
            m, c = band_ref[i, j] * ms[i], band_ref[i, j] * cs[i]
            member, coarse = (m, c) if member is None else (member + m, coarse + c)
        if j < HB:
            down_out[j, :MB] = member.astype(BF16)
            down_out[j, MB:] = coarse.astype(BF16)
        elif j < HB + LV:
            member_out[j - HB] = member
            coarse_out[j - HB] = coarse
        else:
            up_out[j - HB - LV, :MB] = member.astype(BF16)
            up_out[j - HB - LV, MB:] = coarse.astype(BF16)


def finish_kernel(member_ref, coarse_ref, below_ref, above_ref, member_out, coarse_out):
    member_out[HB : LV - HB] = member_ref[HB : LV - HB]
    coarse_out[HB : LV - HB] = coarse_ref[HB : LV - HB]
    for j in range(HB):
        member_out[j] = member_ref[j] + below_ref[j, :MB].astype(F32)
        coarse_out[j] = coarse_ref[j] + below_ref[j, MB:].astype(F32)
        k = LV - HB + j
        member_out[k] = member_ref[k] + above_ref[j, :MB].astype(F32)
        coarse_out[k] = coarse_ref[k] + above_ref[j, MB:].astype(F32)


def shape(dims, kind):
    return jax.ShapeDtypeStruct(dims, kind)


PARAMS = pltpu.CompilerParams(vmem_limit_bytes=24 * 1024 * 1024)


def near(*values):
    return [pltpu.with_memory_space_constraint(value, pltpu.VMEM) for value in values]


def far(*values):
    return [pltpu.with_memory_space_constraint(value, pltpu.HBM) for value in values]


def shards(members_pert, coarse_pert, member_ctrl, coarse_ctrl, vert_loc, stencil, interp_w):
    tiles = lax.axis_size("tile")
    levs = lax.axis_size("lev")
    rising = [(i, i + 1) for i in range(levs - 1)]
    falling = [(j, i) for i, j in rising]
    on_chip = [(i, i ^ 1) for i in range(tiles)]
    off_chip = [(i, (i + 1) % tiles if i % 2 else (i - 1) % tiles) for i in range(tiles)]
    odd = (lax.axis_index("tile") % 2).astype(jnp.int32).reshape(1)
    first_level = lax.axis_index("lev") * LV
    padded = jnp.pad(vert_loc, ((0, 0), (HB, HB)))
    band = lax.dynamic_slice(padded, (first_level, first_level), (LV, WL))

    edge = pltpu.VMEM((HB, MB + CM, ND), BF16)
    held = [pltpu.VMEM(x.shape, x.dtype) for x in (member_ctrl, coarse_ctrl, coarse_pert, stencil, interp_w)]
    hbm = pl.BlockSpec(memory_space=pltpu.HBM)
    top, bottom, member_ctrl, coarse_ctrl, coarse_pert, stencil, interp_w = pl.pallas_call(
        gather_kernel,
        out_shape=(edge, edge, *held),
        in_specs=[hbm] * 5,
        out_specs=(VMEM,) * 7,
        scratch_shapes=[pltpu.SemaphoreType.DMA((9,))],
        compiler_params=PARAMS,
        name="gather",
    )(*far(member_ctrl, coarse_ctrl, coarse_pert, stencil, interp_w))
    below = lax.ppermute(top, "lev", rising)
    above = lax.ppermute(bottom, "lev", falling)
    matrix, pert = pl.pallas_call(
        weights_kernel,
        out_shape=(pltpu.VMEM((SPAN, NF), BF16), pltpu.VMEM((LV * MB, NF), BF16)),
        in_specs=[SMEM, VMEM, VMEM, hbm],
        out_specs=(VMEM, VMEM),
        scratch_shapes=[pltpu.SemaphoreType.DMA],
        cost_estimate=pl.CostEstimate(flops=16 * SPAN * NF, bytes_accessed=2 * SPAN * NF, transcendentals=0),
        compiler_params=PARAMS,
        name="weights",
    )(odd, *near(stencil, interp_w), *far(members_pert.reshape(LV * MB, NF)))
    packed = pltpu.VMEM((HALF, 2 * CW), BF16)
    own, chip, cross = pl.pallas_call(
        localize_kernel,
        out_shape=(pltpu.VMEM((ROWS, ND), BF16), packed, packed),
        in_specs=[SMEM, SMEM, VMEM, VMEM, VMEM, VMEM, VMEM],
        out_specs=(VMEM, VMEM, VMEM),
        scratch_shapes=[pltpu.VMEM((WL, MB, ND), F32), pltpu.VMEM((WL, CM, ND), F32), pltpu.VMEM((2 * HALF, ND), F32)],
        compiler_params=PARAMS,
        name="localize",
    )(odd, band, *near(member_ctrl, coarse_ctrl, below, above, coarse_pert))
    cross = lax.ppermute(cross, "tile", off_chip)
    chip = lax.ppermute(chip, "tile", on_chip)
    own, chip, cross = pl.pallas_call(
        fine_kernel,
        out_shape=(pltpu.VMEM((ROWS, ND), F32), packed, packed),
        in_specs=[VMEM] * 5,
        out_specs=(VMEM, VMEM, VMEM),
        scratch_shapes=[pltpu.VMEM((ROWS, SPAN), BF16)],
        compiler_params=PARAMS,
        name="fine",
    )(*near(own, chip, cross, matrix, pert))
    cross = lax.ppermute(cross, "tile", off_chip)
    chip = lax.ppermute(chip, "tile", on_chip)
    halo = pltpu.VMEM((HB, MB + CM, ND), BF16)
    finals = (shape((LV, MB, ND), F32), shape((LV, CM, ND), F32))
    member, coarse, down, up = pl.pallas_call(
        spread_kernel,
        out_shape=(pltpu.VMEM((LV, MB, ND), F32), pltpu.VMEM((LV, CM, ND), F32), halo, halo),
        in_specs=[SMEM, SMEM, VMEM, VMEM, VMEM, VMEM],
        out_specs=(VMEM, VMEM, VMEM, VMEM),
        scratch_shapes=[pltpu.VMEM((LV, MB, ND), F32), pltpu.VMEM((LV, CM, ND), F32)],
        compiler_params=PARAMS,
        name="spread",
    )(odd, band, *near(own, chip, cross, coarse_pert))
    above = lax.ppermute(down, "lev", falling)
    below = lax.ppermute(up, "lev", rising)
    return pl.pallas_call(
        finish_kernel,
        out_shape=finals,
        in_specs=[VMEM, VMEM, VMEM, VMEM],
        out_specs=(VMEM, VMEM),
        compiler_params=PARAMS,
        name="finish",
    )(*near(member, coarse, below, above))


def solution(mesh):
    block = P("lev", None, "tile")
    in_specs = (block, block, block, block, P(), P(None, "tile"), P(None, "tile"))
    return jax.shard_map(shards, mesh=mesh, in_specs=in_specs, out_specs=(block, block), check_vma=False)
```

```python
import jax
import jax.numpy as jnp
from jax import lax
from jax.experimental import pallas as pl
from jax.experimental.pallas import tpu as pltpu
from jax.sharding import PartitionSpec as P


HB = 4
CW = 64
LV = 16
MB = 16
CM = 8
ND = 256
NF = 4096
WL = LV + 2 * HB
LEVS = 4
BAND = 2 * HB + 1
ROWS = LV * MB + LV
HALF = 144
SPAN = ND + 2 * CW
BLOCK = 512
STEP = 2048
F32 = jnp.float32
BF16 = jnp.bfloat16
VMEM = pl.BlockSpec(memory_space=pltpu.VMEM)


def low_lanes(shape):
    return lax.broadcasted_iota(jnp.int32, shape, 1) < CW


def odd_tile():
    return lax.axis_index("tile") % 2


def odd_lev():
    return lax.axis_index("lev") % 2


def second_half():
    tile = lax.axis_index("tile")
    middle = (tile + 1) // 2 == lax.axis_size("tile") // 4
    return jnp.where(middle, tile % 2, 1 - tile % 2)


def turn(value):
    return pltpu.roll(value, CW, 1)


def run_copies(moves, sems):
    copies = [pltpu.make_async_copy(source, target, sems.at[k]) for k, (source, target) in enumerate(moves)]
    for copy in copies:
        copy.start()
    return copies


def edges_kernel(mc_hbm, cc_hbm, cp_hbm, outer, inner, sems):
    near_first = odd_lev() * (LV - HB)
    far_first = LV - HB - near_first
    moves = []
    for first, target in ((near_first, inner), (far_first, outer)):
        moves.append((mc_hbm.at[pl.ds(first, HB)], target.at[:, pl.ds(0, MB)]))
        moves.append((cc_hbm.at[pl.ds(first, HB)], target.at[:, pl.ds(MB, CM)]))
        moves.append((cp_hbm.at[pl.ds(first, HB)], target.at[:, pl.ds(MB + CM, CM)]))
    for copy in run_copies(moves, sems):
        copy.wait()


def load_kernel(vert_hbm, mc_hbm, cc_hbm, cp_hbm, stencil_hbm, weight_hbm, pert_hbm, ahead_ref, back_ref, mc, cc, cp, stencil, weight, pert, vert, sems):
    moves = [(vert_hbm, vert), (mc_hbm, mc), (cc_hbm, cc), (cp_hbm, cp), (stencil_hbm, stencil), (weight_hbm, weight), (pert_hbm, pert)]
    copies = run_copies(moves, sems)
    first = lax.axis_index("lev") * LV
    final = LV * lax.axis_size("lev") - 1
    copies[0].wait()
    for i in range(LV):
        for d in range(BAND):
            near = first + i
            other = first + i + d - HB
            if i + d < HB:
                other = jnp.maximum(other, 0)
            elif i + d >= HB + LV:
                other = jnp.minimum(other, final)
            ahead_ref[i, d] = jnp.full((8, 128), vert[near, other], F32)
            back_ref[i, d] = jnp.full((8, 128), vert[other, near], F32)
    for copy in copies[1:]:
        copy.wait()


def localize_kernel(band_ref, mc_ref, cc_ref, outer_ref, inner_ref, cp_ref, own_ref, chip_ref, cross_ref, ms, cs, full):
    swapped = odd_lev() == 1
    for j in range(HB):
        outer = outer_ref[j, : MB + CM].astype(F32)
        inner = inner_ref[j, : MB + CM].astype(F32)
        below = jnp.where(swapped, outer, inner)
        above = jnp.where(swapped, inner, outer)
        ms[j], cs[j] = below[:MB], below[MB:]
        ms[HB + LV + j], cs[HB + LV + j] = above[:MB], above[MB:]
    for j in range(LV):
        ms[HB + j] = mc_ref[j].astype(F32)
        cs[HB + j] = cc_ref[j].astype(F32)
    full[ROWS:] = jnp.zeros((2 * HALF - ROWS, ND), F32)
    for i in range(LV):
        member = scaled(band_ref[i, 0], ms[i])
        coarse = scaled(band_ref[i, 0], cs[i])
        for d in range(1, BAND):
            member = member + scaled(band_ref[i, d], ms[i + d])
            coarse = coarse + scaled(band_ref[i, d], cs[i + d])
        full[i * MB : (i + 1) * MB] = member
        coarse = coarse.astype(BF16).astype(F32)
        full[LV * MB + i : LV * MB + i + 1] = jnp.sum(cp_ref[i].astype(F32) * coarse, axis=0, keepdims=True)
    own_ref[...] = full[:ROWS].astype(BF16)
    odd = odd_tile() == 1
    first = full[:, : 2 * CW]
    last = full[:, ND - 2 * CW :]
    low = low_lanes((HALF, 2 * CW))
    first = jnp.where(low, first[:HALF], turn(first[HALF:]))
    last = jnp.where(low, turn(last[:HALF]), last[HALF:])
    cross_ref[...] = jnp.where(odd, last, first).astype(BF16)
    chip_ref[...] = jnp.where(odd, first, last).astype(BF16)


def weights_kernel(stencil_ref, weight_ref, out_ref):
    odd = odd_tile()
    rows = 16
    zero = jnp.zeros((rows, BLOCK), BF16)
    for start in range(0, NF, BLOCK):
        span = pl.ds(start, BLOCK)
        row = lax.broadcasted_iota(jnp.int32, (rows, BLOCK), 0)
        cells = [jnp.broadcast_to(stencil_ref[q : q + 1, span], (rows, BLOCK)) - row for q in range(4)]
        weights = [jnp.broadcast_to(weight_ref[q : q + 1, span].astype(F32), (rows, BLOCK)).astype(BF16) for q in range(4)]
        for low, high, first in ((0, ND, CW), (ND, ND + CW, (1 - odd) * (ND + CW)), (ND + CW, SPAN, odd * (ND + CW))):
            inside = [(cell - first).astype(jnp.int16) for cell in cells]
            for base in range(low, high, rows):
                value = jnp.where(inside[0] == jnp.int16(base - low), weights[0], zero)
                for q in range(1, 4):
                    value = jnp.where(inside[q] == jnp.int16(base - low), weights[q], value)
                out_ref[base : base + rows, span] = value


def scaled(factor, value):
    rows, lanes = value.shape
    return jnp.tile(factor, (rows // 8, lanes // 128)) * value


def fine_kernel(own_ref, chip_ref, cross_ref, matrix_ref, pert, own_out, chip_out, cross_out, field):
    chip = chip_ref[...].astype(F32)
    cross = cross_ref[...].astype(F32)
    low = low_lanes((HALF, 2 * CW))
    field[:, :ND] = own_ref[...]
    field[:HALF, ND:] = jnp.where(low, chip, turn(cross)).astype(BF16)
    field[HALF:, ND:] = jnp.where(low, turn(chip), cross)[: ROWS - HALF].astype(BF16)
    total = jnp.zeros((ROWS, SPAN), F32)
    for b in range(NF // STEP):
        span = pl.ds(b * STEP, STEP)
        matrix = matrix_ref[:, span]
        interp = jnp.dot(field[...], matrix, preferred_element_type=F32)
        member = pert[:, span].astype(F32).reshape(LV, MB, STEP)
        increment = jnp.sum(member * interp[: LV * MB].reshape(LV, MB, STEP), axis=1) + interp[LV * MB :]
        adjoint = (member * increment[:, None, :]).astype(BF16).reshape(LV * MB, STEP)
        adjoint = jnp.concatenate([adjoint, increment.astype(BF16)], axis=0)
        total = total + lax.dot_general(adjoint, matrix, (((1,), (1,)), ((), ())), preferred_element_type=F32)
    own_out[...] = total[:, :ND]
    top = total[:HALF, ND:]
    bottom = jnp.concatenate([total[HALF:, ND:], jnp.zeros((2 * HALF - ROWS, 2 * CW), F32)], axis=0)
    chip_out[...] = jnp.where(low, top, turn(bottom)).astype(BF16)
    cross_out[...] = jnp.where(low, turn(top), bottom).astype(BF16)


def joined(chunk, odd):
    chunk = chunk.astype(F32)
    turned = turn(chunk)
    low = low_lanes((HALF, 2 * CW))
    lead = jnp.concatenate([jnp.where(low, chunk, 0.0), jnp.where(low, turned, 0.0)], axis=0)
    trail = jnp.concatenate([jnp.where(low, 0.0, turned), jnp.where(low, 0.0, chunk)], axis=0)
    return jnp.where(odd, 0.0, lead), jnp.where(odd, trail, 0.0)


def merge_kernel(own_ref, chip_ref, cross_ref, own_out, send_ref):
    here = second_half() * LEVS
    there = LEVS - here
    lev = lax.axis_index("lev")
    for k in range(LEVS):
        send_ref[there + k] = cross_ref[...]
    lead, trail = joined(chip_ref[...], odd_tile() == 0)
    own_out[:, : 2 * CW] = own_ref[:, : 2 * CW] + lead[:ROWS]
    own_out[:, 2 * CW :] = own_ref[:, 2 * CW :] + trail[:ROWS]
    edge = HB * MB
    blank = jnp.zeros((HALF - 2 * edge - 2 * HB, 2 * CW), F32)
    for first, place in ((0, jnp.maximum(lev - 1, 0)), (LV - HB, jnp.minimum(lev + 1, LEVS - 1))):
        rows = slice(first * MB, first * MB + edge)
        row = slice(LV * MB + first, LV * MB + first + HB)
        parts = [own_out[rows, : 2 * CW], own_out[rows, 2 * CW :], own_out[row, : 2 * CW], own_out[row, 2 * CW :], blank]
        send_ref[here + place] = jnp.concatenate(parts, axis=0).astype(BF16)


def finish_kernel(band_ref, own_ref, got_ref, cp_ref, outer_ref, inner_ref, member_hbm, coarse_hbm, ms, cs, member_out, coarse_out, sems):
    odd = odd_tile() == 1
    swapped = odd_lev() == 1
    here = second_half() * LEVS
    there = LEVS - here
    lev = lax.axis_index("lev")
    lower = jnp.maximum(lev - 1, 0)
    upper = jnp.minimum(lev + 1, LEVS - 1)
    wide = 2 * CW
    edge = HB * MB
    lead, trail = joined(got_ref[there + lev], odd)
    for i in range(LV):
        rows = slice(i * MB, (i + 1) * MB)
        row = slice(LV * MB + i, LV * MB + i + 1)
        ms[HB + i, :, :wide] = own_ref[rows, :wide] + lead[rows]
        ms[HB + i, :, wide:] = own_ref[rows, wide:] + trail[rows]
        pert = cp_ref[i].astype(F32)
        cs[HB + i, :, :wide] = pert[:, :wide] * (own_ref[row, :wide] + lead[row])
        cs[HB + i, :, wide:] = pert[:, wide:] * (own_ref[row, wide:] + trail[row])
    for place, first, base, below in ((lower, LV - HB, 0, swapped), (upper, 0, HB + LV, ~swapped)):
        lead, trail = joined(got_ref[there + place], odd)
        near = got_ref[here + place].astype(F32)
        near = jnp.where(place == lev, 0.0, near)
        lead = jnp.where(place == lev, 0.0, lead)
        trail = jnp.where(place == lev, 0.0, trail)
        for w in range(HB):
            rows = slice((first + w) * MB, (first + w + 1) * MB)
            row = slice(LV * MB + first + w, LV * MB + first + w + 1)
            ms[base + w, :, :wide] = near[w * MB : (w + 1) * MB] + lead[rows]
            ms[base + w, :, wide:] = near[edge + w * MB : edge + (w + 1) * MB] + trail[rows]
            pert = jnp.where(below, outer_ref[w, MB + CM :].astype(F32), inner_ref[w, MB + CM :].astype(F32))
            k = 2 * edge + w
            cs[base + w, :, :wide] = pert[:, :wide] * (near[k : k + 1] + lead[row])
            cs[base + w, :, wide:] = pert[:, wide:] * (near[k + HB : k + HB + 1] + trail[row])
    copies = []
    for j in range(LV):
        member = scaled(band_ref[j, 0], ms[j])
        coarse = scaled(band_ref[j, 0], cs[j])
        for d in range(1, BAND):
            member = member + scaled(band_ref[j, d], ms[j + d])
            coarse = coarse + scaled(band_ref[j, d], cs[j + d])
        member_out[j] = member
        coarse_out[j] = coarse
        if j % HB == HB - 1:
            span = pl.ds(j + 1 - HB, HB)
            for source, target in ((member_out, member_hbm), (coarse_out, coarse_hbm)):
                copies.append(pltpu.make_async_copy(source.at[span], target.at[span], sems.at[len(copies)]))
                copies[-1].start()
    for copy in copies:
        copy.wait()


def shape(dims, kind):
    return jax.ShapeDtypeStruct(dims, kind)


PARAMS = pltpu.CompilerParams(vmem_limit_bytes=24 * 1024 * 1024)


def near(*values):
    return [pltpu.with_memory_space_constraint(value, pltpu.VMEM) for value in values]


def far(*values):
    return [pltpu.with_memory_space_constraint(value, pltpu.HBM) for value in values]


def shards(members_pert, coarse_pert, member_ctrl, coarse_ctrl, vert_loc, stencil, interp_w):
    tiles = lax.axis_size("tile")
    levs = lax.axis_size("lev")
    outer_pairs = [(i, i ^ 1) for i in range(levs)]
    inner_pairs = [(1, 2), (2, 1)]
    on_chip = [(i, i ^ 1) for i in range(tiles)]
    off_chip = [(i, (i + 1) % tiles if i % 2 else (i - 1) % tiles) for i in range(tiles)]
    edge = pltpu.VMEM((HB, MB + 2 * CM, ND), BF16)
    hbm = pl.BlockSpec(memory_space=pltpu.HBM)
    outer, inner = pl.pallas_call(
        edges_kernel,
        out_shape=(edge, edge),
        in_specs=[hbm] * 3,
        out_specs=(VMEM, VMEM),
        scratch_shapes=[pltpu.SemaphoreType.DMA((6,))],
        compiler_params=PARAMS,
        name="edges",
    )(*far(member_ctrl, coarse_ctrl, coarse_pert))
    inner = lax.ppermute(inner, "lev", inner_pairs)
    outer = lax.ppermute(outer, "lev", outer_pairs)
    splats = pltpu.VMEM((LV, BAND, 8, 128), F32)
    values = (member_ctrl, coarse_ctrl, coarse_pert, stencil, interp_w, members_pert.reshape(LV * MB, NF))
    ahead, back, member_ctrl, coarse_ctrl, coarse_pert, stencil, interp_w, pert = pl.pallas_call(
        load_kernel,
        out_shape=(splats, splats, *[pltpu.VMEM(x.shape, x.dtype) for x in values]),
        in_specs=[hbm] * 7,
        out_specs=(VMEM,) * 8,
        scratch_shapes=[pltpu.SMEM(vert_loc.shape, F32), pltpu.SemaphoreType.DMA((7,))],
        compiler_params=PARAMS,
        name="load",
    )(*far(vert_loc, *values))
    matrix = pl.pallas_call(
        weights_kernel,
        out_shape=pltpu.VMEM((SPAN, NF), BF16),
        in_specs=[VMEM, VMEM],
        out_specs=VMEM,
        cost_estimate=pl.CostEstimate(flops=16 * SPAN * NF, bytes_accessed=2 * SPAN * NF, transcendentals=0),
        compiler_params=PARAMS,
        name="weights",
    )(*near(stencil, interp_w))
    packed = pltpu.VMEM((HALF, 2 * CW), BF16)
    own, chip, cross = pl.pallas_call(
        localize_kernel,
        out_shape=(pltpu.VMEM((ROWS, ND), BF16), packed, packed),
        in_specs=[VMEM] * 6,
        out_specs=(VMEM, VMEM, VMEM),
        scratch_shapes=[pltpu.VMEM((WL, MB, ND), F32), pltpu.VMEM((WL, CM, ND), F32), pltpu.VMEM((2 * HALF, ND), F32)],
        compiler_params=PARAMS,
        name="localize",
    )(*near(ahead, member_ctrl, coarse_ctrl, outer, inner, coarse_pert))
    cross = lax.ppermute(cross, "tile", off_chip)
    chip = lax.ppermute(chip, "tile", on_chip)
    own, chip, cross = pl.pallas_call(
        fine_kernel,
        out_shape=(pltpu.VMEM((ROWS, ND), F32), packed, packed),
        in_specs=[VMEM] * 5,
        out_specs=(VMEM, VMEM, VMEM),
        scratch_shapes=[pltpu.VMEM((ROWS, SPAN), BF16)],
        compiler_params=PARAMS,
        name="fine",
    )(*near(own, chip, cross, matrix, pert))
    chip = lax.ppermute(chip, "tile", on_chip)
    own, send = pl.pallas_call(
        merge_kernel,
        out_shape=(pltpu.VMEM((ROWS, ND), F32), pltpu.VMEM((2 * LEVS, HALF, 2 * CW), BF16)),
        in_specs=[VMEM, VMEM, VMEM],
        out_specs=(VMEM, VMEM),
        compiler_params=PARAMS,
        name="merge",
    )(*near(own, chip, cross))
    pairs = [(t, (t + 1) % tiles) if t + 1 != tiles // 2 else (t + 1, t) for t in range(1, tiles, 2)]
    groups = [[t * levs + z for t in pair for z in range(levs)] for pair in pairs]
    got = lax.all_to_all(send, ("tile", "lev"), 0, 0, axis_index_groups=groups)
    finals = (shape((LV, MB, ND), F32), shape((LV, CM, ND), F32))
    return pl.pallas_call(
        finish_kernel,
        out_shape=finals,
        in_specs=[VMEM] * 6,
        out_specs=(hbm, hbm),
        scratch_shapes=[
            pltpu.VMEM((WL, MB, ND), F32),
            pltpu.VMEM((WL, CM, ND), F32),
            pltpu.VMEM((LV, MB, ND), F32),
            pltpu.VMEM((LV, CM, ND), F32),
            pltpu.SemaphoreType.DMA((2 * LV // HB,)),
        ],
        compiler_params=PARAMS,
        name="finish",
    )(*near(back, own, got, coarse_pert, outer, inner))


def solution(mesh):
    block = P("lev", None, "tile")
    in_specs = (block, block, block, block, P(), P(None, "tile"), P(None, "tile"))
    return jax.shard_map(shards, mesh=mesh, in_specs=in_specs, out_specs=(block, block), check_vma=False)
```

```python
import jax
import jax.numpy as jnp
from jax import lax
from jax.experimental import pallas as pl
from jax.experimental.pallas import tpu as pltpu
from jax.sharding import PartitionSpec as P


HB = 4
CW = 64
LV = 16
MB = 16
CM = 8
ND = 256
NF = 4096
WL = LV + 2 * HB
LEVS = 4
LEAD = 1
BAND = 2 * HB + 1
ROWS = LV * MB + LV
HALF = 144
SPAN = ND + 2 * CW
BLOCK = 512
STEP = 2048
F32 = jnp.float32
BF16 = jnp.bfloat16
VMEM = pl.BlockSpec(memory_space=pltpu.VMEM)


def low_lanes(shape):
    return lax.broadcasted_iota(jnp.int32, shape, 1) < CW


def odd_tile():
    return lax.axis_index("tile") % 2


def slot(lev):
    return (lev + LEVS - LEAD) % LEVS


def odd_lev():
    return lax.axis_index("lev") % 2


def second_half():
    tile = lax.axis_index("tile")
    middle = (tile + 1) // 2 == lax.axis_size("tile") // 4
    return jnp.where(middle, tile % 2, 1 - tile % 2)


def turn(value):
    return pltpu.roll(value, CW, 1)


def run_copies(moves, sems):
    copies = [pltpu.make_async_copy(source, target, sems.at[k]) for k, (source, target) in enumerate(moves)]
    for copy in copies:
        copy.start()
    return copies


def edges_kernel(mc_hbm, cc_hbm, cp_hbm, outer, inner, sems):
    near_first = odd_lev() * (LV - HB)
    far_first = LV - HB - near_first
    moves = []
    for first, target in ((near_first, inner), (far_first, outer)):
        moves.append((mc_hbm.at[pl.ds(first, HB)], target.at[:, pl.ds(0, MB)]))
        moves.append((cc_hbm.at[pl.ds(first, HB)], target.at[:, pl.ds(MB, CM)]))
        moves.append((cp_hbm.at[pl.ds(first, HB)], target.at[:, pl.ds(MB + CM, CM)]))
    for copy in run_copies(moves, sems):
        copy.wait()


def load_kernel(vert_hbm, mc_hbm, cc_hbm, cp_hbm, stencil_hbm, weight_hbm, pert_hbm, ahead_ref, back_ref, mc, cc, cp, stencil, weight, pert, vert, sems):
    moves = [(vert_hbm, vert), (mc_hbm, mc), (cc_hbm, cc), (cp_hbm, cp), (stencil_hbm, stencil), (weight_hbm, weight), (pert_hbm, pert)]
    copies = run_copies(moves, sems)
    first = lax.axis_index("lev") * LV
    final = LV * lax.axis_size("lev") - 1
    copies[0].wait()
    for i in range(LV):
        for d in range(BAND):
            near = first + i
            other = first + i + d - HB
            if i + d < HB:
                other = jnp.maximum(other, 0)
            elif i + d >= HB + LV:
                other = jnp.minimum(other, final)
            ahead_ref[i, d] = jnp.full((8, 128), vert[near, other], F32)
            back_ref[i, d] = jnp.full((8, 128), vert[other, near], F32)
    for copy in copies[1:]:
        copy.wait()


def localize_kernel(band_ref, mc_ref, cc_ref, outer_ref, inner_ref, cp_ref, own_ref, chip_ref, cross_ref, ms, cs, full):
    swapped = odd_lev() == 1
    for j in range(HB):
        outer = outer_ref[j, : MB + CM].astype(F32)
        inner = inner_ref[j, : MB + CM].astype(F32)
        below = jnp.where(swapped, outer, inner)
        above = jnp.where(swapped, inner, outer)
        ms[j], cs[j] = below[:MB], below[MB:]
        ms[HB + LV + j], cs[HB + LV + j] = above[:MB], above[MB:]
    for j in range(LV):
        ms[HB + j] = mc_ref[j].astype(F32)
        cs[HB + j] = cc_ref[j].astype(F32)
    full[ROWS:] = jnp.zeros((2 * HALF - ROWS, ND), F32)
    for i in range(LV):
        member = scaled(band_ref[i, 0], ms[i])
        coarse = scaled(band_ref[i, 0], cs[i])
        for d in range(1, BAND):
            member = member + scaled(band_ref[i, d], ms[i + d])
            coarse = coarse + scaled(band_ref[i, d], cs[i + d])
        full[i * MB : (i + 1) * MB] = member
        coarse = coarse.astype(BF16).astype(F32)
        full[LV * MB + i : LV * MB + i + 1] = jnp.sum(cp_ref[i].astype(F32) * coarse, axis=0, keepdims=True)
    own_ref[...] = full[:ROWS].astype(BF16)
    odd = odd_tile() == 1
    first = full[:, : 2 * CW]
    last = full[:, ND - 2 * CW :]
    low = low_lanes((HALF, 2 * CW))
    first = jnp.where(low, first[:HALF], turn(first[HALF:]))
    last = jnp.where(low, turn(last[:HALF]), last[HALF:])
    cross_ref[...] = jnp.where(odd, last, first).astype(BF16)
    chip_ref[...] = jnp.where(odd, first, last).astype(BF16)


def weights_kernel(stencil_ref, weight_ref, out_ref):
    odd = odd_tile()
    rows = 16
    zero = jnp.zeros((rows, BLOCK), BF16)
    for start in range(0, NF, BLOCK):
        span = pl.ds(start, BLOCK)
        row = lax.broadcasted_iota(jnp.int32, (rows, BLOCK), 0)
        cells = [jnp.broadcast_to(stencil_ref[q : q + 1, span], (rows, BLOCK)) - row for q in range(4)]
        weights = [jnp.broadcast_to(weight_ref[q : q + 1, span].astype(F32), (rows, BLOCK)).astype(BF16) for q in range(4)]
        for low, high, first in ((0, ND, CW), (ND, ND + CW, (1 - odd) * (ND + CW)), (ND + CW, SPAN, odd * (ND + CW))):
            inside = [(cell - first).astype(jnp.int16) for cell in cells]
            for base in range(low, high, rows):
                value = jnp.where(inside[0] == jnp.int16(base - low), weights[0], zero)
                for q in range(1, 4):
                    value = jnp.where(inside[q] == jnp.int16(base - low), weights[q], value)
                out_ref[base : base + rows, span] = value


def scaled(factor, value):
    rows, lanes = value.shape
    return jnp.tile(factor, (rows // 8, lanes // 128)) * value


def fine_kernel(own_ref, chip_ref, cross_ref, matrix_ref, pert, own_out, chip_out, cross_out, field):
    chip = chip_ref[...].astype(F32)
    cross = cross_ref[...].astype(F32)
    low = low_lanes((HALF, 2 * CW))
    field[:, :ND] = own_ref[...]
    field[:HALF, ND:] = jnp.where(low, chip, turn(cross)).astype(BF16)
    field[HALF:, ND:] = jnp.where(low, turn(chip), cross)[: ROWS - HALF].astype(BF16)
    total = jnp.zeros((ROWS, SPAN), F32)
    for b in range(NF // STEP):
        span = pl.ds(b * STEP, STEP)
        matrix = matrix_ref[:, span]
        interp = jnp.dot(field[...], matrix, preferred_element_type=F32)
        member = pert[:, span].astype(F32).reshape(LV, MB, STEP)
        increment = jnp.sum(member * interp[: LV * MB].reshape(LV, MB, STEP), axis=1) + interp[LV * MB :]
        adjoint = (member * increment[:, None, :]).astype(BF16).reshape(LV * MB, STEP)
        adjoint = jnp.concatenate([adjoint, increment.astype(BF16)], axis=0)
        total = total + lax.dot_general(adjoint, matrix, (((1,), (1,)), ((), ())), preferred_element_type=F32)
    own_out[...] = total[:, :ND]
    top = total[:HALF, ND:]
    bottom = jnp.concatenate([total[HALF:, ND:], jnp.zeros((2 * HALF - ROWS, 2 * CW), F32)], axis=0)
    chip_out[...] = jnp.where(low, top, turn(bottom)).astype(BF16)
    cross_out[...] = jnp.where(low, turn(top), bottom).astype(BF16)


def joined(chunk, odd):
    chunk = chunk.astype(F32)
    turned = turn(chunk)
    low = low_lanes((HALF, 2 * CW))
    lead = jnp.concatenate([jnp.where(low, chunk, 0.0), jnp.where(low, turned, 0.0)], axis=0)
    trail = jnp.concatenate([jnp.where(low, 0.0, turned), jnp.where(low, 0.0, chunk)], axis=0)
    return jnp.where(odd, 0.0, lead), jnp.where(odd, trail, 0.0)


def merge_kernel(own_ref, chip_ref, cross_ref, own_out, send_ref):
    here = second_half() * LEVS
    there = LEVS - here
    lev = lax.axis_index("lev")
    for k in range(LEVS):
        send_ref[there + k] = cross_ref[...]
    lead, trail = joined(chip_ref[...], odd_tile() == 0)
    own_out[:, : 2 * CW] = own_ref[:, : 2 * CW] + lead[:ROWS]
    own_out[:, 2 * CW :] = own_ref[:, 2 * CW :] + trail[:ROWS]
    edge = HB * MB
    blank = jnp.zeros((HALF - 2 * edge - 2 * HB, 2 * CW), F32)
    for first, place in ((0, jnp.maximum(lev - 1, 0)), (LV - HB, jnp.minimum(lev + 1, LEVS - 1))):
        rows = slice(first * MB, first * MB + edge)
        row = slice(LV * MB + first, LV * MB + first + HB)
        parts = [own_out[rows, : 2 * CW], own_out[rows, 2 * CW :], own_out[row, : 2 * CW], own_out[row, 2 * CW :], blank]
        send_ref[here + slot(place)] = jnp.concatenate(parts, axis=0).astype(BF16)


def finish_kernel(band_ref, own_ref, got_ref, cp_ref, outer_ref, inner_ref, member_hbm, coarse_hbm, ms, cs, member_out, coarse_out, sems):
    odd = odd_tile() == 1
    swapped = odd_lev() == 1
    here = second_half() * LEVS
    there = LEVS - here
    lev = lax.axis_index("lev")
    lower = jnp.maximum(lev - 1, 0)
    upper = jnp.minimum(lev + 1, LEVS - 1)
    wide = 2 * CW
    edge = HB * MB
    lead, trail = joined(got_ref[there + slot(lev)], odd)
    for i in range(LV):
        rows = slice(i * MB, (i + 1) * MB)
        row = slice(LV * MB + i, LV * MB + i + 1)
        ms[HB + i, :, :wide] = own_ref[rows, :wide] + lead[rows]
        ms[HB + i, :, wide:] = own_ref[rows, wide:] + trail[rows]
        pert = cp_ref[i].astype(F32)
        cs[HB + i, :, :wide] = pert[:, :wide] * (own_ref[row, :wide] + lead[row])
        cs[HB + i, :, wide:] = pert[:, wide:] * (own_ref[row, wide:] + trail[row])
    for place, first, base, below in ((lower, LV - HB, 0, swapped), (upper, 0, HB + LV, ~swapped)):
        lead, trail = joined(got_ref[there + slot(place)], odd)
        near = got_ref[here + slot(place)].astype(F32)
        near = jnp.where(place == lev, 0.0, near)
        lead = jnp.where(place == lev, 0.0, lead)
        trail = jnp.where(place == lev, 0.0, trail)
        for w in range(HB):
            rows = slice((first + w) * MB, (first + w + 1) * MB)
            row = slice(LV * MB + first + w, LV * MB + first + w + 1)
            ms[base + w, :, :wide] = near[w * MB : (w + 1) * MB] + lead[rows]
            ms[base + w, :, wide:] = near[edge + w * MB : edge + (w + 1) * MB] + trail[rows]
            pert = jnp.where(below, outer_ref[w, MB + CM :].astype(F32), inner_ref[w, MB + CM :].astype(F32))
            k = 2 * edge + w
            cs[base + w, :, :wide] = pert[:, :wide] * (near[k : k + 1] + lead[row])
            cs[base + w, :, wide:] = pert[:, wide:] * (near[k + HB : k + HB + 1] + trail[row])
    copies = []
    for j in range(LV):
        member = scaled(band_ref[j, 0], ms[j])
        coarse = scaled(band_ref[j, 0], cs[j])
        for d in range(1, BAND):
            member = member + scaled(band_ref[j, d], ms[j + d])
            coarse = coarse + scaled(band_ref[j, d], cs[j + d])
        member_out[j] = member
        coarse_out[j] = coarse
        if j % HB == HB - 1:
            span = pl.ds(j + 1 - HB, HB)
            for source, target in ((member_out, member_hbm), (coarse_out, coarse_hbm)):
                copies.append(pltpu.make_async_copy(source.at[span], target.at[span], sems.at[len(copies)]))
                copies[-1].start()
    for copy in copies:
        copy.wait()


def shape(dims, kind):
    return jax.ShapeDtypeStruct(dims, kind)


PARAMS = pltpu.CompilerParams(vmem_limit_bytes=24 * 1024 * 1024)


def near(*values):
    return [pltpu.with_memory_space_constraint(value, pltpu.VMEM) for value in values]


def far(*values):
    return [pltpu.with_memory_space_constraint(value, pltpu.HBM) for value in values]


def shards(members_pert, coarse_pert, member_ctrl, coarse_ctrl, vert_loc, stencil, interp_w):
    tiles = lax.axis_size("tile")
    levs = lax.axis_size("lev")
    outer_pairs = [(i, i ^ 1) for i in range(levs)]
    inner_pairs = [(1, 2), (2, 1)]
    on_chip = [(i, i ^ 1) for i in range(tiles)]
    off_chip = [(i, (i + 1) % tiles if i % 2 else (i - 1) % tiles) for i in range(tiles)]
    edge = pltpu.VMEM((HB, MB + 2 * CM, ND), BF16)
    hbm = pl.BlockSpec(memory_space=pltpu.HBM)
    outer, inner = pl.pallas_call(
        edges_kernel,
        out_shape=(edge, edge),
        in_specs=[hbm] * 3,
        out_specs=(VMEM, VMEM),
        scratch_shapes=[pltpu.SemaphoreType.DMA((6,))],
        compiler_params=PARAMS,
        name="edges",
    )(*far(member_ctrl, coarse_ctrl, coarse_pert))
    inner = lax.ppermute(inner, "lev", inner_pairs)
    outer = lax.ppermute(outer, "lev", outer_pairs)
    splats = pltpu.VMEM((LV, BAND, 8, 128), F32)
    values = (member_ctrl, coarse_ctrl, coarse_pert, stencil, interp_w, members_pert.reshape(LV * MB, NF))
    ahead, back, member_ctrl, coarse_ctrl, coarse_pert, stencil, interp_w, pert = pl.pallas_call(
        load_kernel,
        out_shape=(splats, splats, *[pltpu.VMEM(x.shape, x.dtype) for x in values]),
        in_specs=[hbm] * 7,
        out_specs=(VMEM,) * 8,
        scratch_shapes=[pltpu.SMEM(vert_loc.shape, F32), pltpu.SemaphoreType.DMA((7,))],
        compiler_params=PARAMS,
        name="load",
    )(*far(vert_loc, *values))
    matrix = pl.pallas_call(
        weights_kernel,
        out_shape=pltpu.VMEM((SPAN, NF), BF16),
        in_specs=[VMEM, VMEM],
        out_specs=VMEM,
        cost_estimate=pl.CostEstimate(flops=16 * SPAN * NF, bytes_accessed=2 * SPAN * NF, transcendentals=0),
        compiler_params=PARAMS,
        name="weights",
    )(*near(stencil, interp_w))
    packed = pltpu.VMEM((HALF, 2 * CW), BF16)
    own, chip, cross = pl.pallas_call(
        localize_kernel,
        out_shape=(pltpu.VMEM((ROWS, ND), BF16), packed, packed),
        in_specs=[VMEM] * 6,
        out_specs=(VMEM, VMEM, VMEM),
        scratch_shapes=[pltpu.VMEM((WL, MB, ND), F32), pltpu.VMEM((WL, CM, ND), F32), pltpu.VMEM((2 * HALF, ND), F32)],
        compiler_params=PARAMS,
        name="localize",
    )(*near(ahead, member_ctrl, coarse_ctrl, outer, inner, coarse_pert))
    cross = lax.ppermute(cross, "tile", off_chip)
    chip = lax.ppermute(chip, "tile", on_chip)
    own, chip, cross = pl.pallas_call(
        fine_kernel,
        out_shape=(pltpu.VMEM((ROWS, ND), F32), packed, packed),
        in_specs=[VMEM] * 5,
        out_specs=(VMEM, VMEM, VMEM),
        scratch_shapes=[pltpu.VMEM((ROWS, SPAN), BF16)],
        compiler_params=PARAMS,
        name="fine",
    )(*near(own, chip, cross, matrix, pert))
    chip = lax.ppermute(chip, "tile", on_chip)
    own, send = pl.pallas_call(
        merge_kernel,
        out_shape=(pltpu.VMEM((ROWS, ND), F32), pltpu.VMEM((2 * LEVS, HALF, 2 * CW), BF16)),
        in_specs=[VMEM, VMEM, VMEM],
        out_specs=(VMEM, VMEM),
        compiler_params=PARAMS,
        name="merge",
    )(*near(own, chip, cross))
    pairs = [(t, (t + 1) % tiles) if t + 1 != tiles // 2 else (t + 1, t) for t in range(1, tiles, 2)]
    groups = [[t * levs + (z + LEAD) % levs for t in pair for z in range(levs)] for pair in pairs]
    got = lax.all_to_all(send, ("tile", "lev"), 0, 0, axis_index_groups=groups)
    finals = (shape((LV, MB, ND), F32), shape((LV, CM, ND), F32))
    return pl.pallas_call(
        finish_kernel,
        out_shape=finals,
        in_specs=[VMEM] * 6,
        out_specs=(hbm, hbm),
        scratch_shapes=[
            pltpu.VMEM((WL, MB, ND), F32),
            pltpu.VMEM((WL, CM, ND), F32),
            pltpu.VMEM((LV, MB, ND), F32),
            pltpu.VMEM((LV, CM, ND), F32),
            pltpu.SemaphoreType.DMA((2 * LV // HB,)),
        ],
        compiler_params=PARAMS,
        name="finish",
    )(*near(back, own, got, coarse_pert, outer, inner))


def solution(mesh):
    block = P("lev", None, "tile")
    in_specs = (block, block, block, block, P(), P(None, "tile"), P(None, "tile"))
    return jax.shard_map(shards, mesh=mesh, in_specs=in_specs, out_specs=(block, block), check_vma=False)
```

```python
import jax
import jax.numpy as jnp
from jax import lax
from jax.experimental import pallas as pl
from jax.experimental.pallas import tpu as pltpu
from jax.sharding import PartitionSpec as P


HB = 4
CW = 64
LV = 16
MB = 16
CM = 8
ND = 256
NF = 4096
WL = LV + 2 * HB
LEVS = 4
LEAD = 1
BAND = 2 * HB + 1
ROWS = LV * MB + LV
HALF = 144
SPAN = ND + 2 * CW
BLOCK = 512
STEP = 2048
OUT = 2
F32 = jnp.float32
BF16 = jnp.bfloat16
VMEM = pl.BlockSpec(memory_space=pltpu.VMEM)


def low_lanes(shape):
    return lax.broadcasted_iota(jnp.int32, shape, 1) < CW


def odd_tile():
    return lax.axis_index("tile") % 2


def slot(lev):
    return (lev + LEVS - LEAD) % LEVS


def odd_lev():
    return lax.axis_index("lev") % 2


def second_half():
    tile = lax.axis_index("tile")
    middle = (tile + 1) // 2 == lax.axis_size("tile") // 4
    return jnp.where(middle, tile % 2, 1 - tile % 2)


def turn(value):
    return pltpu.roll(value, CW, 1)


def run_copies(moves, sems):
    copies = [pltpu.make_async_copy(source, target, sems.at[k]) for k, (source, target) in enumerate(moves)]
    for copy in copies:
        copy.start()
    return copies


def edges_kernel(mc_hbm, cc_hbm, cp_hbm, outer, inner, sems):
    near_first = odd_lev() * (LV - HB)
    far_first = LV - HB - near_first
    moves = []
    for first, target in ((near_first, inner), (far_first, outer)):
        moves.append((mc_hbm.at[pl.ds(first, HB)], target.at[:, pl.ds(0, MB)]))
        moves.append((cc_hbm.at[pl.ds(first, HB)], target.at[:, pl.ds(MB, CM)]))
        moves.append((cp_hbm.at[pl.ds(first, HB)], target.at[:, pl.ds(MB + CM, CM)]))
    for copy in run_copies(moves, sems):
        copy.wait()


def load_kernel(vert_hbm, mc_hbm, cc_hbm, cp_hbm, stencil_hbm, weight_hbm, pert_hbm, ahead_ref, back_ref, mc, cc, cp, stencil, weight, pert, vert, sems):
    moves = [(vert_hbm, vert), (mc_hbm, mc), (cc_hbm, cc), (cp_hbm, cp), (stencil_hbm, stencil), (weight_hbm, weight), (pert_hbm, pert)]
    copies = run_copies(moves, sems)
    first = lax.axis_index("lev") * LV
    final = LV * lax.axis_size("lev") - 1
    copies[0].wait()
    for i in range(LV):
        for d in range(BAND):
            near = first + i
            other = first + i + d - HB
            if i + d < HB:
                other = jnp.maximum(other, 0)
            elif i + d >= HB + LV:
                other = jnp.minimum(other, final)
            ahead_ref[i, d] = jnp.full((8, 128), vert[near, other], F32)
            back_ref[i, d] = jnp.full((8, 128), vert[other, near], F32)
    for copy in copies[1:]:
        copy.wait()


def localize_kernel(band_ref, mc_ref, cc_ref, outer_ref, inner_ref, cp_ref, own_ref, chip_ref, cross_ref, ms, cs, full):
    swapped = odd_lev() == 1
    for j in range(HB):
        outer = outer_ref[j, : MB + CM].astype(F32)
        inner = inner_ref[j, : MB + CM].astype(F32)
        below = jnp.where(swapped, outer, inner)
        above = jnp.where(swapped, inner, outer)
        ms[j], cs[j] = below[:MB], below[MB:]
        ms[HB + LV + j], cs[HB + LV + j] = above[:MB], above[MB:]
    for j in range(LV):
        ms[HB + j] = mc_ref[j].astype(F32)
        cs[HB + j] = cc_ref[j].astype(F32)
    full[ROWS:] = jnp.zeros((2 * HALF - ROWS, ND), F32)
    for i in range(LV):
        member = scaled(band_ref[i, 0], ms[i])
        coarse = scaled(band_ref[i, 0], cs[i])
        for d in range(1, BAND):
            member = member + scaled(band_ref[i, d], ms[i + d])
            coarse = coarse + scaled(band_ref[i, d], cs[i + d])
        full[i * MB : (i + 1) * MB] = member
        coarse = coarse.astype(BF16).astype(F32)
        full[LV * MB + i : LV * MB + i + 1] = jnp.sum(cp_ref[i].astype(F32) * coarse, axis=0, keepdims=True)
    own_ref[...] = full[:ROWS].astype(BF16)
    odd = odd_tile() == 1
    first = full[:, : 2 * CW]
    last = full[:, ND - 2 * CW :]
    low = low_lanes((HALF, 2 * CW))
    first = jnp.where(low, first[:HALF], turn(first[HALF:]))
    last = jnp.where(low, turn(last[:HALF]), last[HALF:])
    cross_ref[...] = jnp.where(odd, last, first).astype(BF16)
    chip_ref[...] = jnp.where(odd, first, last).astype(BF16)


def weights_kernel(stencil_ref, weight_ref, out_ref):
    odd = odd_tile()
    rows = 16
    zero = jnp.zeros((rows, BLOCK), BF16)
    for start in range(0, NF, BLOCK):
        span = pl.ds(start, BLOCK)
        row = lax.broadcasted_iota(jnp.int32, (rows, BLOCK), 0)
        cells = [jnp.broadcast_to(stencil_ref[q : q + 1, span], (rows, BLOCK)) - row for q in range(4)]
        weights = [jnp.broadcast_to(weight_ref[q : q + 1, span].astype(F32), (rows, BLOCK)).astype(BF16) for q in range(4)]
        for low, high, first in ((0, ND, CW), (ND, ND + CW, (1 - odd) * (ND + CW)), (ND + CW, SPAN, odd * (ND + CW))):
            inside = [(cell - first).astype(jnp.int16) for cell in cells]
            for base in range(low, high, rows):
                value = jnp.where(inside[0] == jnp.int16(base - low), weights[0], zero)
                for q in range(1, 4):
                    value = jnp.where(inside[q] == jnp.int16(base - low), weights[q], value)
                out_ref[base : base + rows, span] = value


def scaled(factor, value):
    rows, lanes = value.shape
    return jnp.tile(factor, (rows // 8, lanes // 128)) * value


def fine_kernel(own_ref, chip_ref, cross_ref, matrix_ref, pert, own_out, chip_out, cross_out, field):
    chip = chip_ref[...].astype(F32)
    cross = cross_ref[...].astype(F32)
    low = low_lanes((HALF, 2 * CW))
    field[:, :ND] = own_ref[...]
    field[:HALF, ND:] = jnp.where(low, chip, turn(cross)).astype(BF16)
    field[HALF:, ND:] = jnp.where(low, turn(chip), cross)[: ROWS - HALF].astype(BF16)
    total = jnp.zeros((ROWS, SPAN), F32)
    for b in range(NF // STEP):
        span = pl.ds(b * STEP, STEP)
        matrix = matrix_ref[:, span]
        interp = jnp.dot(field[...], matrix, preferred_element_type=F32)
        member = pert[:, span].astype(F32).reshape(LV, MB, STEP)
        increment = jnp.sum(member * interp[: LV * MB].reshape(LV, MB, STEP), axis=1) + interp[LV * MB :]
        adjoint = (member * increment[:, None, :]).astype(BF16).reshape(LV * MB, STEP)
        adjoint = jnp.concatenate([adjoint, increment.astype(BF16)], axis=0)
        total = total + lax.dot_general(adjoint, matrix, (((1,), (1,)), ((), ())), preferred_element_type=F32)
    own_out[...] = total[:, :ND]
    top = total[:HALF, ND:]
    bottom = jnp.concatenate([total[HALF:, ND:], jnp.zeros((2 * HALF - ROWS, 2 * CW), F32)], axis=0)
    chip_out[...] = jnp.where(low, top, turn(bottom)).astype(BF16)
    cross_out[...] = jnp.where(low, turn(top), bottom).astype(BF16)


def joined(chunk, odd):
    chunk = chunk.astype(F32)
    turned = turn(chunk)
    low = low_lanes((HALF, 2 * CW))
    lead = jnp.concatenate([jnp.where(low, chunk, 0.0), jnp.where(low, turned, 0.0)], axis=0)
    trail = jnp.concatenate([jnp.where(low, 0.0, turned), jnp.where(low, 0.0, chunk)], axis=0)
    return jnp.where(odd, 0.0, lead), jnp.where(odd, trail, 0.0)


def merge_kernel(own_ref, chip_ref, cross_ref, own_out, send_ref):
    here = second_half() * LEVS
    there = LEVS - here
    lev = lax.axis_index("lev")
    for k in range(LEVS):
        send_ref[there + k] = cross_ref[...]
    lead, trail = joined(chip_ref[...], odd_tile() == 0)
    own_out[:, : 2 * CW] = own_ref[:, : 2 * CW] + lead[:ROWS]
    own_out[:, 2 * CW :] = own_ref[:, 2 * CW :] + trail[:ROWS]
    edge = HB * MB
    blank = jnp.zeros((HALF - 2 * edge - 2 * HB, 2 * CW), F32)
    for first, place in ((0, jnp.maximum(lev - 1, 0)), (LV - HB, jnp.minimum(lev + 1, LEVS - 1))):
        rows = slice(first * MB, first * MB + edge)
        row = slice(LV * MB + first, LV * MB + first + HB)
        parts = [own_out[rows, : 2 * CW], own_out[rows, 2 * CW :], own_out[row, : 2 * CW], own_out[row, 2 * CW :], blank]
        send_ref[here + slot(place)] = jnp.concatenate(parts, axis=0).astype(BF16)


def finish_kernel(band_ref, own_ref, got_ref, cp_ref, outer_ref, inner_ref, member_hbm, coarse_hbm, ms, cs, member_out, coarse_out, sems):
    odd = odd_tile() == 1
    swapped = odd_lev() == 1
    here = second_half() * LEVS
    there = LEVS - here
    lev = lax.axis_index("lev")
    lower = jnp.maximum(lev - 1, 0)
    upper = jnp.minimum(lev + 1, LEVS - 1)
    wide = 2 * CW
    edge = HB * MB
    lead, trail = joined(got_ref[there + slot(lev)], odd)
    for i in range(LV):
        rows = slice(i * MB, (i + 1) * MB)
        row = slice(LV * MB + i, LV * MB + i + 1)
        ms[HB + i, :, :wide] = own_ref[rows, :wide] + lead[rows]
        ms[HB + i, :, wide:] = own_ref[rows, wide:] + trail[rows]
        pert = cp_ref[i].astype(F32)
        cs[HB + i, :, :wide] = pert[:, :wide] * (own_ref[row, :wide] + lead[row])
        cs[HB + i, :, wide:] = pert[:, wide:] * (own_ref[row, wide:] + trail[row])
    for place, first, base, below in ((lower, LV - HB, 0, swapped), (upper, 0, HB + LV, ~swapped)):
        lead, trail = joined(got_ref[there + slot(place)], odd)
        near = got_ref[here + slot(place)].astype(F32)
        near = jnp.where(place == lev, 0.0, near)
        lead = jnp.where(place == lev, 0.0, lead)
        trail = jnp.where(place == lev, 0.0, trail)
        for w in range(HB):
            rows = slice((first + w) * MB, (first + w + 1) * MB)
            row = slice(LV * MB + first + w, LV * MB + first + w + 1)
            ms[base + w, :, :wide] = near[w * MB : (w + 1) * MB] + lead[rows]
            ms[base + w, :, wide:] = near[edge + w * MB : edge + (w + 1) * MB] + trail[rows]
            pert = jnp.where(below, outer_ref[w, MB + CM :].astype(F32), inner_ref[w, MB + CM :].astype(F32))
            k = 2 * edge + w
            cs[base + w, :, :wide] = pert[:, :wide] * (near[k : k + 1] + lead[row])
            cs[base + w, :, wide:] = pert[:, wide:] * (near[k + HB : k + HB + 1] + trail[row])
    copies = []
    for j in range(LV):
        member = scaled(band_ref[j, 0], ms[j])
        coarse = scaled(band_ref[j, 0], cs[j])
        for d in range(1, BAND):
            member = member + scaled(band_ref[j, d], ms[j + d])
            coarse = coarse + scaled(band_ref[j, d], cs[j + d])
        member_out[j] = member
        coarse_out[j] = coarse
        if j % OUT == OUT - 1:
            span = pl.ds(j + 1 - OUT, OUT)
            for source, target in ((member_out, member_hbm), (coarse_out, coarse_hbm)):
                copies.append(pltpu.make_async_copy(source.at[span], target.at[span], sems.at[len(copies)]))
                copies[-1].start()
    for copy in copies:
        copy.wait()


def shape(dims, kind):
    return jax.ShapeDtypeStruct(dims, kind)


PARAMS = pltpu.CompilerParams(vmem_limit_bytes=24 * 1024 * 1024)


def near(*values):
    return [pltpu.with_memory_space_constraint(value, pltpu.VMEM) for value in values]


def far(*values):
    return [pltpu.with_memory_space_constraint(value, pltpu.HBM) for value in values]


def shards(members_pert, coarse_pert, member_ctrl, coarse_ctrl, vert_loc, stencil, interp_w):
    tiles = lax.axis_size("tile")
    levs = lax.axis_size("lev")
    outer_pairs = [(i, i ^ 1) for i in range(levs)]
    inner_pairs = [(1, 2), (2, 1)]
    on_chip = [(i, i ^ 1) for i in range(tiles)]
    off_chip = [(i, (i + 1) % tiles if i % 2 else (i - 1) % tiles) for i in range(tiles)]
    edge = pltpu.VMEM((HB, MB + 2 * CM, ND), BF16)
    hbm = pl.BlockSpec(memory_space=pltpu.HBM)
    outer, inner = pl.pallas_call(
        edges_kernel,
        out_shape=(edge, edge),
        in_specs=[hbm] * 3,
        out_specs=(VMEM, VMEM),
        scratch_shapes=[pltpu.SemaphoreType.DMA((6,))],
        compiler_params=PARAMS,
        name="edges",
    )(*far(member_ctrl, coarse_ctrl, coarse_pert))
    inner = lax.ppermute(inner, "lev", inner_pairs)
    outer = lax.ppermute(outer, "lev", outer_pairs)
    splats = pltpu.VMEM((LV, BAND, 8, 128), F32)
    values = (member_ctrl, coarse_ctrl, coarse_pert, stencil, interp_w, members_pert.reshape(LV * MB, NF))
    ahead, back, member_ctrl, coarse_ctrl, coarse_pert, stencil, interp_w, pert = pl.pallas_call(
        load_kernel,
        out_shape=(splats, splats, *[pltpu.VMEM(x.shape, x.dtype) for x in values]),
        in_specs=[hbm] * 7,
        out_specs=(VMEM,) * 8,
        scratch_shapes=[pltpu.SMEM(vert_loc.shape, F32), pltpu.SemaphoreType.DMA((7,))],
        compiler_params=PARAMS,
        name="load",
    )(*far(vert_loc, *values))
    matrix = pl.pallas_call(
        weights_kernel,
        out_shape=pltpu.VMEM((SPAN, NF), BF16),
        in_specs=[VMEM, VMEM],
        out_specs=VMEM,
        cost_estimate=pl.CostEstimate(flops=16 * SPAN * NF, bytes_accessed=2 * SPAN * NF, transcendentals=0),
        compiler_params=PARAMS,
        name="weights",
    )(*near(stencil, interp_w))
    packed = pltpu.VMEM((HALF, 2 * CW), BF16)
    own, chip, cross = pl.pallas_call(
        localize_kernel,
        out_shape=(pltpu.VMEM((ROWS, ND), BF16), packed, packed),
        in_specs=[VMEM] * 6,
        out_specs=(VMEM, VMEM, VMEM),
        scratch_shapes=[pltpu.VMEM((WL, MB, ND), F32), pltpu.VMEM((WL, CM, ND), F32), pltpu.VMEM((2 * HALF, ND), F32)],
        compiler_params=PARAMS,
        name="localize",
    )(*near(ahead, member_ctrl, coarse_ctrl, outer, inner, coarse_pert))
    cross = lax.ppermute(cross, "tile", off_chip)
    chip = lax.ppermute(chip, "tile", on_chip)
    own, chip, cross = pl.pallas_call(
        fine_kernel,
        out_shape=(pltpu.VMEM((ROWS, ND), F32), packed, packed),
        in_specs=[VMEM] * 5,
        out_specs=(VMEM, VMEM, VMEM),
        scratch_shapes=[pltpu.VMEM((ROWS, SPAN), BF16)],
        compiler_params=PARAMS,
        name="fine",
    )(*near(own, chip, cross, matrix, pert))
    chip = lax.ppermute(chip, "tile", on_chip)
    own, send = pl.pallas_call(
        merge_kernel,
        out_shape=(pltpu.VMEM((ROWS, ND), F32), pltpu.VMEM((2 * LEVS, HALF, 2 * CW), BF16)),
        in_specs=[VMEM, VMEM, VMEM],
        out_specs=(VMEM, VMEM),
        compiler_params=PARAMS,
        name="merge",
    )(*near(own, chip, cross))
    pairs = [(t, (t + 1) % tiles) if t + 1 != tiles // 2 else (t + 1, t) for t in range(1, tiles, 2)]
    groups = [[t * levs + (z + LEAD) % levs for t in pair for z in range(levs)] for pair in pairs]
    got = lax.all_to_all(send, ("tile", "lev"), 0, 0, axis_index_groups=groups)
    finals = (shape((LV, MB, ND), F32), shape((LV, CM, ND), F32))
    return pl.pallas_call(
        finish_kernel,
        out_shape=finals,
        in_specs=[VMEM] * 6,
        out_specs=(hbm, hbm),
        scratch_shapes=[
            pltpu.VMEM((WL, MB, ND), F32),
            pltpu.VMEM((WL, CM, ND), F32),
            pltpu.VMEM((LV, MB, ND), F32),
            pltpu.VMEM((LV, CM, ND), F32),
            pltpu.SemaphoreType.DMA((2 * LV // OUT,)),
        ],
        compiler_params=PARAMS,
        name="finish",
    )(*near(back, own, got, coarse_pert, outer, inner))


def solution(mesh):
    block = P("lev", None, "tile")
    in_specs = (block, block, block, block, P(), P(None, "tile"), P(None, "tile"))
    return jax.shard_map(shards, mesh=mesh, in_specs=in_specs, out_specs=(block, block), check_vma=False)
```
